32 devices in a mesh: groups: 2 (over y), ep: 4 (over z), tp: 4 (over x, core).
Axes of the slice: x: 2, y: 2, z: 4, core: 2. Of those that a mesh axis runs over, the one named last changes fastest.
Arguments:
- tokens: bfloat16 [1024, 2560], P(('groups', 'ep')), parts along dimension 0, may hold values from -6 to 6
- device_choice: int32 [1024, 3], P(('groups', 'ep')), parts along dimension 0, may hold values from 0 to 3, as said below
- local_expert: int32 [1024, 6], P(('groups', 'ep')), parts along dimension 0, may hold values from 0 to 1, as said below
- route_weight: float32 [1024, 6], P(('groups', 'ep')), parts along dimension 0, may hold values from 0.1 to 1
- prefill_ranks: int32 [4], P('groups'), parts along dimension 0, may hold values from 0 to 3, as said below
- w_gate: bfloat16 [8, 1024, 2560], P('ep', 'tp'), may hold values from -0.125 to 0.125
- w_up: bfloat16 [8, 1024, 2560], P('ep', 'tp'), may hold values from -0.125 to 0.125
- w_down: bfloat16 [8, 1024, 2560], P('ep', 'tp'), may hold values from -0.1875 to 0.1875
Outputs:
- moe_out: bfloat16 [1024, 2560], P(('groups', 'ep', 'tp')), parts along dimension 0
The draws below stay inside these ranges and needn't reach their ends.
There are 2 independent parts, one for each index of `groups`. The reference program is written for one: setup_inputs(seed, part) draws one part's arguments, and reference() takes and returns one part's arrays. A program takes and returns all parts, laid end to end along the dimension named above; an argument that names none is the same for every part. Nothing has to cross between parts.
Inputs may be any that keep to these rules, and one draw needn't show every extreme that they name: `device_choice`: each row names 3 different ranks. The rows of one rank (aligned blocks of 128 rows) name any one rank at most 96 times, and every block names some rank exactly 96 times. `local_expert`: picks 2k and 2k + 1 of a row are two different experts of the rank in column k of device_choice. So the rows of one rank choose one expert at most 96 times, and some expert is chosen exactly 96 times by the rows of every rank. `prefill_ranks`: 2 different ranks.
All inputs are finite; a program needn't handle non-finite values.
Results may differ from the reference program's by a relative error of at most 0.014.
Values may be sent and summed in bfloat16 or wider, within the bound.
A program may use at most 128 MiB of HBM per device.

```python
import math
import jax
import jax.numpy as jnp
from jax import lax

D = 2560
F = 1024
EXP_DEV = 2
TOPK = 6
DEV_TOP = 3
DEC_RANK = 8
EXPERTS = 8
RANK_ROWS = 128
PRE_RANKS = 2
ROWS = 512
CAP = 96
N_EP = 4
N_TP = 4


def route_draw(key):
    base_key = jax.random.fold_in(key, 101)
    key_star, key_local, key_order, key_rows, key_first, key_second, key_swap = jax.random.split(base_key, 7)
    star_rank = jax.random.randint(key_star, (), 0, N_EP).astype(jnp.int32)
    star_local = jax.random.randint(key_local, (), 0, EXP_DEV).astype(jnp.int32)
    others = jax.vmap(lambda one_key: jax.random.permutation(one_key, N_EP - 1))(jax.random.split(key_order, N_EP))
    rank_order = jnp.concatenate([jnp.full((N_EP, 1), star_rank, jnp.int32), (star_rank + 1 + others.astype(jnp.int32)) % N_EP], axis=1)
    row_order = jax.vmap(lambda one_key: jax.random.permutation(one_key, RANK_ROWS))(jax.random.split(key_rows, N_EP))
    cycle_pos = (DEV_TOP * row_order.astype(jnp.int32)[:, :, None] + jnp.arange(DEV_TOP, dtype=jnp.int32)[None, None, :]) % N_EP
    chosen = jnp.take_along_axis(rank_order, cycle_pos.reshape(N_EP, RANK_ROWS * DEV_TOP), axis=1)
    chosen = chosen.reshape(N_EP * RANK_ROWS, DEV_TOP).astype(jnp.int32)
    pick_shape = (N_EP * RANK_ROWS, DEV_TOP)
    first_pick = jax.random.randint(key_first, pick_shape, 0, EXP_DEV).astype(jnp.int32)
    first_pick = jnp.where(chosen == star_rank, star_local, first_pick)
    second = (first_pick + 1 + jax.random.randint(key_second, pick_shape, 0, EXP_DEV - 1).astype(jnp.int32)) % EXP_DEV
    swap_bits = jax.random.randint(key_swap, pick_shape, 0, 2)
    pick_one = jnp.where(swap_bits == 1, second, first_pick)
    pick_two = jnp.where(swap_bits == 1, first_pick, second)
    local_picks = jnp.stack([pick_one, pick_two], axis=2).reshape(N_EP * RANK_ROWS, 2 * DEV_TOP)
    return (chosen, local_picks.astype(jnp.int32))


def draw_device_choice(key, part):
    chosen, local_picks = route_draw(key)
    return chosen


def draw_local_expert(key, part):
    chosen, local_picks = route_draw(key)
    return local_picks


def draw_prefill_ranks(key, part):
    shuffled = jax.random.permutation(jax.random.fold_in(key, 211), N_EP)
    return shuffled[:PRE_RANKS].astype(jnp.int32)


def block_scale(rng, shape, shards, low, top_value):
    def one(axis_at, parts):
        steps = jax.random.uniform(jax.random.fold_in(jax.random.fold_in(rng, 6), axis_at), (parts,), jnp.float32, low / len(shards), top_value / len(shards))
        return jnp.repeat(jnp.exp(steps), shape[axis_at] // parts).reshape((-1,) + (1,) * (len(shape) - axis_at - 1))

    gain = one(*shards[0])
    for cut in shards[1:]:
        gain = gain * one(*cut)
    return gain


def centred(rng, extent, scale, limit, cuts=(), kind=jnp.bfloat16):
    level = block_scale(rng, extent, cuts, -0.22, 0.18) if cuts else 1.0
    values = jax.random.normal(rng, extent, jnp.float32) * scale * level
    return jnp.minimum(jnp.maximum(values, -limit), limit).astype(kind)


def setup_inputs(seed: int = 0, part: int = 0) -> dict:
    streams_of = jax.random.split(jax.random.key(seed), 9)
    part_splits = jax.random.split(jax.random.fold_in(streams_of[8], part), 9)
    return {
        "tokens": centred(part_splits[0], (ROWS, D), 1.0, 6.0, ((0, 4),)),
        "device_choice": draw_device_choice(jax.random.fold_in(jax.random.fold_in(streams_of[8], part), 71), part),
        "local_expert": draw_local_expert(jax.random.fold_in(jax.random.fold_in(streams_of[8], part), 71), part),
        "route_weight": jnp.clip(jnp.exp(math.log(1.0) - 2.3025851 * jax.random.uniform(part_splits[3], (ROWS, TOPK), jnp.float32) ** block_scale(part_splits[3], (ROWS, TOPK), ((0, 4),), -0.2, 0.2)), 0.1, 1.0),
        "prefill_ranks": draw_prefill_ranks(jax.random.fold_in(jax.random.fold_in(streams_of[8], part), 71), part),
        "w_gate": centred(streams_of[5], (EXPERTS, F, D), D ** -0.5, 0.125, ((0, 4), (1, 4))),
        "w_up": centred(streams_of[6], (EXPERTS, F, D), D ** -0.5, 0.125, ((0, 4), (1, 4))),
        "w_down": centred(streams_of[7], (EXPERTS, F, D), F ** -0.5, 0.1875, ((0, 4), (1, 4))),
    }


def reference(tokens, device_choice, local_expert, route_weight, prefill_ranks, w_gate, w_up, w_down):
    row_count = tokens.shape[0]
    row_ids = jnp.arange(row_count, dtype=jnp.int32)
    rank_of = row_ids // RANK_ROWS
    in_prefill = jnp.any(rank_of[:, None] == prefill_ranks[None, :], axis=1)
    is_live = (row_ids % RANK_ROWS < DEC_RANK) | in_prefill
    expert_id = jnp.repeat(device_choice, 2, axis=1) * EXP_DEV + local_expert
    weights = jnp.where(is_live[:, None], route_weight, jnp.zeros_like(route_weight))
    most_rows = N_EP * CAP
    group_width = F // N_TP

    def per_expert(totals, expert):
        matches = (expert_id == expert) & is_live[:, None]
        picked = jnp.any(matches, axis=1)
        chosen_weight = jnp.sum(jnp.where(matches, weights, jnp.zeros_like(weights)), axis=1)
        row_index = jnp.nonzero(picked, size=most_rows, fill_value=row_count)[0].astype(jnp.int32)
        safe_index = jnp.minimum(row_index, row_count - 1).astype(jnp.int32)
        gathered = tokens[safe_index]
        gate_w = lax.dynamic_index_in_dim(w_gate, expert, 0, keepdims=False)
        up_w = lax.dynamic_index_in_dim(w_up, expert, 0, keepdims=False)
        down_w = lax.dynamic_index_in_dim(w_down, expert, 0, keepdims=False)
        gate_act = jnp.dot(gathered, gate_w.T, preferred_element_type=jnp.float32)
        up_act = jnp.dot(gathered, up_w.T, preferred_element_type=jnp.float32)
        hidden = (jax.nn.silu(gate_act) * up_act).astype(jnp.bfloat16)
        summed = jnp.zeros((most_rows, tokens.shape[1]), jnp.float32)
        for group in range(N_TP):
            low = group * group_width
            part_sum = jnp.dot(hidden[:, low:low + group_width], down_w[low:low + group_width], preferred_element_type=jnp.float32)
            summed = summed + part_sum.astype(jnp.bfloat16).astype(jnp.float32)
        weighted = chosen_weight[safe_index][:, None] * summed
        totals = totals.at[row_index].add(weighted, mode="drop")
        return totals, None

    zeros_init = jnp.zeros((row_count, tokens.shape[1]), jnp.float32)
    totals, unused = lax.scan(per_expert, zeros_init, jnp.arange(EXPERTS, dtype=jnp.int32))
    return totals.astype(jnp.bfloat16)
```

```python
import functools

import jax
import jax.numpy as jnp
from jax import lax
from jax.experimental import pallas as pl
from jax.experimental.pallas import tpu as pltpu
from jax.sharding import PartitionSpec as P

TOPK = 6
DEV_TOP = 3
DEC_RANK = 8
LANES = 128
CORES = 2
VMEM_BYTES = 67_043_328
MESH = pl.DeviceIdType.MESH


def count_slots(slot_keys, is_live, bin_count):
    hits = (
        slot_keys[:, :, None] == jnp.arange(bin_count, dtype=jnp.int32)[None, None, :]
    ) & is_live[:, None, None]
    flat_hits = hits.astype(jnp.int32).reshape(-1, bin_count)
    before = jnp.cumsum(flat_hits, axis=0) - flat_hits
    return jnp.sum(before * flat_hits, axis=1).reshape(slot_keys.shape)


def by_collectives(
    tokens, device_choice, local_expert, route_weight, prefill_ranks, w_gate, w_up, w_down
):
    rank_count = lax.axis_size("ep")
    own_rank = lax.axis_index("ep")
    rank_rows = tokens.shape[0]
    model_width = tokens.shape[1]
    experts_here = w_gate.shape[0]
    capacity = (DEV_TOP * rank_rows + rank_count - 1) // rank_count
    row_ids = jnp.arange(rank_rows, dtype=jnp.int32)
    is_live = (row_ids < DEC_RANK) | jnp.any(prefill_ranks == own_rank)
    pair_rank = jnp.repeat(device_choice, 2, axis=1)
    expert_keys = pair_rank * experts_here + local_expert
    positions = count_slots(device_choice, is_live, rank_count)
    send_ids = device_choice * capacity + positions
    send_count = rank_count * capacity
    pick_index = expert_keys * capacity + jnp.repeat(positions, 2, axis=1)
    block_shape = (rank_count, 1, capacity, model_width)
    slot_ids = jnp.arange(send_count, dtype=jnp.int32)
    select = jnp.any(
        (send_ids[None, :, :] == slot_ids[:, None, None]) & is_live[None, :, None], axis=2
    ).astype(jnp.bfloat16)
    outgoing = (
        jnp.dot(select, tokens, preferred_element_type=jnp.float32)
        .astype(jnp.bfloat16)
        .reshape(block_shape)
    )
    blocks = lax.all_to_all(outgoing, "ep", split_axis=0, concat_axis=0, tiled=True)
    gate_act = jnp.einsum("scd,efd->secf", blocks[:, 0], w_gate, preferred_element_type=jnp.float32)
    up_act = jnp.einsum("scd,efd->secf", blocks[:, 0], w_up, preferred_element_type=jnp.float32)
    hidden = (jax.nn.silu(gate_act) * up_act).astype(jnp.bfloat16)
    partial_value = jnp.einsum(
        "secf,efd->secd", hidden, w_down, preferred_element_type=jnp.float32
    ).astype(jnp.bfloat16)
    returned = lax.all_to_all(partial_value, "ep", split_axis=0, concat_axis=0, tiled=True)
    back_width = returned.shape[3]
    flat_back = returned.reshape(-1, back_width)
    weights = jnp.where(is_live[:, None], route_weight, jnp.zeros_like(route_weight))
    shares = jnp.zeros((rank_rows, back_width), jnp.float32)
    for pick_slot in range(TOPK):
        picked_rows = flat_back[pick_index[:, pick_slot]].astype(jnp.float32)
        shares = shares + weights[:, pick_slot : pick_slot + 1] * picked_rows
    summed = lax.psum_scatter(shares.astype(jnp.bfloat16), "tp", scatter_dimension=0, tiled=True)
    return summed


def fused_kernel(
    ranks, pairs, tokens, own_weights, w_gate, w_up, w_down, out,
    rows_in, mix, gate, up, down, total, half_out, half_in, side_out, side_in, far_out, far_in,
    load_sem, mix_send, mix_recv, z_send, z_recv, x_send, x_recv, c_send, c_recv,
    half_send, half_recv, side_send, side_recv, far_send, far_recv,
):
    me = lax.axis_index("ep")
    spot = lax.axis_index("tp")
    column, core = spot // CORES, spot % CORES
    partner = column * CORES + (1 - core)
    experts, hidden_here, width = w_gate.shape
    pieces, piece_rows = rows_in.shape[1], rows_in.shape[2]
    rank_rows = pieces * piece_rows

    def at_column(step):
        return ((column + step) % pairs) * CORES + core

    loads = [
        pltpu.make_async_copy(tokens, rows_in.at[me], load_sem.at[0]),
        pltpu.make_async_copy(own_weights.at[me], mix.at[me], load_sem.at[1]),
        pltpu.make_async_copy(w_gate, gate, load_sem.at[2]),
        pltpu.make_async_copy(w_up, up, load_sem.at[3]),
        pltpu.make_async_copy(w_down, down, load_sem.at[4]),
    ]
    for load in loads:
        load.start()

    barrier = pltpu.get_barrier_semaphore()
    for step in range(1, ranks):
        pl.semaphore_signal(
            barrier, inc=1, device_id={"ep": (me + step) % ranks}, device_id_type=MESH
        )
    for step in range(1, pairs):
        pl.semaphore_signal(barrier, inc=1, device_id={"tp": at_column(step)}, device_id_type=MESH)
    pl.semaphore_signal(barrier, inc=1, device_id={"tp": partner}, device_id_type=MESH)
    pl.semaphore_wait(barrier, ranks - 1 + pairs - 1 + 1)

    def remote(src, dst, send, recv, target):
        return pltpu.make_async_remote_copy(
            src_ref=src, dst_ref=dst, send_sem=send, recv_sem=recv,
            device_id=target, device_id_type=MESH,
        )

    def mix_copy(step):
        other = (me + step) % ranks
        return remote(
            own_weights.at[other], mix.at[me], mix_send.at[step - 1], mix_recv.at[me], {"ep": other}
        )

    def z_copy(block, way):
        piece = rows_in.at[block, spot]
        other = me + 1 if way == 0 else me - 1
        return remote(piece, piece, z_send.at[way, block], z_recv.at[block], {"ep": other})

    def x_copy(block, step):
        piece = rows_in.at[block, spot]
        return remote(
            piece, piece, x_send.at[block, step - 1], x_recv.at[block, step - 1],
            {"tp": at_column(step)},
        )

    def c_copy(block, step):
        piece = rows_in.at[block, at_column(pairs - step)]
        return remote(
            piece, piece, c_send.at[block, step], c_recv.at[block, step], {"tp": partner}
        )

    def half_copy(block):
        return remote(
            half_out.at[block], half_in.at[block], half_send.at[block], half_recv.at[block],
            {"tp": partner},
        )

    def side_copy(block, step):
        return remote(
            side_out.at[block, step - 1], side_in.at[block, step - 1],
            side_send.at[block, step - 1], side_recv.at[block, step - 1],
            {"tp": at_column(step)},
        )

    def far_copy(block):
        return remote(
            far_out.at[block], far_in.at[me], far_send.at[block], far_recv.at[me], {"ep": block}
        )

    def far_arrival(block):
        return remote(
            far_out.at[block], far_in.at[block], far_send.at[block], far_recv.at[block],
            {"ep": block},
        )

    def mix_arrival(block):
        return remote(
            own_weights.at[block], mix.at[block], mix_send.at[0], mix_recv.at[block], {"ep": block}
        )

    def passes(block, way):
        if way == 0:
            return (block <= me) & (me + 1 < ranks)
        return (block >= me) & (me > 0)

    def onward(block):
        for way in range(2):
            @pl.when(passes(block, way))
            def _():
                z_copy(block, way).start()

    near = jnp.minimum(me, ranks - 1 - me)

    def nth(i):
        alternating = jnp.where(i % 2 == 1, me - (i + 1) // 2, me + i // 2)
        rest = jnp.where(me <= near, i, ranks - 1 - i)
        return jnp.where(i <= 2 * near, alternating, rest)

    def arrive(i):
        block = nth(i)
        z_copy(block, 0).wait_recv()
        onward(block)
        for step in range(1, pairs):
            x_copy(block, step).start()
        c_copy(block, 0).start()

    def across(i):
        block = nth(i)
        for step in range(1, pairs):
            x_copy(block, step).wait_recv()
            c_copy(block, step).start()

    def compute(i):
        block = nth(i)

        @pl.when(i > 0)
        def _():
            for step in range(pairs):
                c_copy(block, step).wait_recv()
            mix_arrival(block).wait_recv()

        rows = rows_in[block].reshape(rank_rows, width)
        hidden = []
        for expert in range(experts):
            by_row = (((1,), (1,)), ((), ()))
            gate_act = lax.dot_general(rows, gate[expert], by_row, preferred_element_type=jnp.float32)
            up_act = lax.dot_general(rows, up[expert], by_row, preferred_element_type=jnp.float32)
            scale = jnp.broadcast_to(mix[block, pl.ds(expert, 1), :], (LANES, rank_rows)).T
            scale = jnp.concatenate([scale] * (hidden_here // LANES), axis=1)
            act = gate_act / (1.0 + jnp.exp(-gate_act)) * up_act * scale
            hidden.append(act.astype(jnp.bfloat16))
        hidden = jnp.concatenate(hidden, axis=1)
        tile = 512 if width % 512 == 0 else LANES
        for low in range(0, width, tile):
            part = jnp.dot(
                hidden,
                down[:, :, low : low + tile].reshape(experts * hidden_here, tile),
                preferred_element_type=jnp.float32,
            )
            total[block, :, :, low : low + tile] = part.reshape(pieces, piece_rows, tile)
        for col in range(pairs):
            half_out[block, col] = total[block, col * CORES + (1 - core)].astype(jnp.bfloat16)
        half_copy(block).start()

    def merge_half(i):
        block = nth(i)
        half_copy(block).wait_recv()
        for step in range(1, pairs):
            place = at_column(step)
            both = total[block, place] + half_in[block, (column + step) % pairs].astype(jnp.float32)
            side_out[block, step - 1] = both.astype(jnp.bfloat16)
            side_copy(block, step).start()
        total[block, spot] = total[block, spot] + half_in[block, column].astype(jnp.float32)

    def merge_side(i):
        block = nth(i)
        acc = total[block, spot]
        for step in range(1, pairs):
            side_copy(block, step).wait_recv()
            acc = acc + side_in[block, step - 1].astype(jnp.float32)

        @pl.when(i > 0)
        def _():
            far_out[block] = acc.astype(jnp.bfloat16)
            far_copy(block).start()

        @pl.when(i == 0)
        def _():
            total[block, spot] = acc

    loads[0].wait()
    onward(me)
    for step in range(1, ranks):
        mix_copy(step).start()
    for load in loads[1:]:
        load.wait()

    @pl.loop(0, ranks)
    def _(i):
        compute(i)

        @pl.when(i == 0)
        def _():
            if ranks > 1:
                arrive(1)
            merge_half(0)

        @pl.when(i + 2 < ranks)
        def _():
            arrive(i + 2)

        @pl.when(i > 0)
        def _():
            merge_half(i)
            merge_side(i - 1)

        @pl.when(i + 1 < ranks)
        def _():
            across(i + 1)

    merge_side(ranks - 1)
    acc = total[me, spot]
    for step in range(1, ranks):
        block = nth(step)
        far_arrival(block).wait_recv()
        acc = acc + far_in[block].astype(jnp.float32)
    out[...] = acc.astype(out.dtype)

    @pl.loop(0, ranks)
    def _(i):
        block = nth(i)
        for way in range(2):
            @pl.when(passes(block, way))
            def _():
                z_copy(block, way).wait_send()
        half_copy(block).wait_send()
        for step in range(1, pairs):
            side_copy(block, step).wait_send()

        @pl.when(i > 0)
        def _():
            for step in range(1, pairs):
                x_copy(block, step).wait_send()
            for step in range(pairs):
                c_copy(block, step).wait_send()
            far_copy(block).wait_send()

    for step in range(1, ranks):
        mix_copy(step).wait_send()


def scratch_of(ranks, pairs, experts, rank_rows, hidden_here, width):
    pieces = pairs * CORES
    piece_rows = rank_rows // pieces
    sub = max(8, experts)
    arrays = [
        ((ranks, pieces, piece_rows, width), jnp.bfloat16),
        ((ranks, sub, rank_rows), jnp.float32),
        ((experts, hidden_here, width), jnp.bfloat16),
        ((experts, hidden_here, width), jnp.bfloat16),
        ((experts, hidden_here, width), jnp.bfloat16),
        ((ranks, pieces, piece_rows, width), jnp.float32),
        ((ranks, pairs, piece_rows, width), jnp.bfloat16),
        ((ranks, pairs, piece_rows, width), jnp.bfloat16),
        ((ranks, pairs - 1, piece_rows, width), jnp.bfloat16),
        ((ranks, pairs - 1, piece_rows, width), jnp.bfloat16),
        ((ranks, piece_rows, width), jnp.bfloat16),
        ((ranks, piece_rows, width), jnp.bfloat16),
    ]
    sems = [
        (5,), (max(ranks - 1, 1),), (ranks,), (2, ranks), (ranks,),
        (ranks, pairs - 1), (ranks, pairs - 1), (ranks, pairs), (ranks, pairs),
        (ranks,), (ranks,), (ranks, pairs - 1), (ranks, pairs - 1), (ranks,), (ranks,),
    ]
    return arrays, sems


def byte_count(arrays):
    total = 0
    for shape, kind in arrays:
        size = jnp.dtype(kind).itemsize
        for extent in shape:
            size *= extent
        total += size
    return total


def on_device(
    tokens, device_choice, local_expert, route_weight, prefill_ranks, w_gate, w_up, w_down
):
    ranks = lax.axis_size("ep")
    spots = lax.axis_size("tp")
    rank_rows, width = tokens.shape
    experts, hidden_here, _ = w_gate.shape
    pairs = spots // CORES
    fits = False
    if (
        ranks > 1 and pairs > 1 and spots % CORES == 0 and rank_rows % (spots * 16) == 0
        and rank_rows % LANES == 0 and hidden_here % LANES == 0 and width % LANES == 0
    ):
        arrays, sems = scratch_of(ranks, pairs, experts, rank_rows, hidden_here, width)
        fits = byte_count(arrays) < VMEM_BYTES * 3 // 4
    if not fits:
        return by_collectives(
            tokens, device_choice, local_expert, route_weight, prefill_ranks, w_gate, w_up, w_down
        )
    own_rank = lax.axis_index("ep")
    row_ids = jnp.arange(rank_rows, dtype=jnp.int32)
    is_live = (row_ids < DEC_RANK) | jnp.any(prefill_ranks == own_rank)
    weights = jnp.where(is_live[:, None], route_weight, jnp.zeros_like(route_weight))
    expert_id = jnp.repeat(device_choice, 2, axis=1) * experts + local_expert
    all_ids = jnp.arange(ranks * experts, dtype=jnp.int32)
    own_weights = jnp.sum(
        jnp.where(expert_id[None, :, :] == all_ids[:, None, None], weights[None, :, :], 0.0), axis=2
    ).reshape(ranks, experts, rank_rows)
    sub = max(8, experts)
    own_weights = jnp.pad(own_weights, ((0, 0), (0, sub - experts), (0, 0)))
    piece_rows = rank_rows // spots
    anywhere = pl.BlockSpec(memory_space=pl.ANY)
    in_vmem = pl.BlockSpec(memory_space=pltpu.VMEM)
    return pl.pallas_call(
        functools.partial(fused_kernel, ranks, pairs),
        out_shape=jax.ShapeDtypeStruct((piece_rows, width), jnp.bfloat16),
        in_specs=[anywhere, in_vmem, anywhere, anywhere, anywhere],
        out_specs=in_vmem,
        scratch_shapes=[pltpu.VMEM(shape, kind) for shape, kind in arrays]
        + [pltpu.SemaphoreType.DMA(shape) for shape in sems],
        compiler_params=pltpu.CompilerParams(
            collective_id=0, has_side_effects=True, vmem_limit_bytes=VMEM_BYTES * 15 // 16
        ),
    )(tokens.reshape(spots, piece_rows, width), own_weights, w_gate, w_up, w_down)


def solution(mesh):
    in_specs = (
        P(("groups", "ep"), None),
        P(("groups", "ep"), None),
        P(("groups", "ep"), None),
        P(("groups", "ep"), None),
        P("groups"),
        P("ep", "tp", None),
        P("ep", "tp", None),
        P("ep", "tp", None),
    )
    out_specs = P(("groups", "ep", "tp"), None)
    return jax.shard_map(
        on_device, mesh=mesh, in_specs=in_specs, out_specs=out_specs, check_vma=False
    )
```

```python
import functools

import jax
import jax.numpy as jnp
from jax import lax
from jax.experimental import pallas as pl
from jax.experimental.pallas import tpu as pltpu
from jax.sharding import PartitionSpec as P

TOPK = 6
DEV_TOP = 3
DEC_RANK = 8
LANES = 128
CORES = 2
VMEM_BYTES = 67_043_328
PARTS = 2
MESH = pl.DeviceIdType.MESH


def count_slots(slot_keys, is_live, bin_count):
    hits = (
        slot_keys[:, :, None] == jnp.arange(bin_count, dtype=jnp.int32)[None, None, :]
    ) & is_live[:, None, None]
    flat_hits = hits.astype(jnp.int32).reshape(-1, bin_count)
    before = jnp.cumsum(flat_hits, axis=0) - flat_hits
    return jnp.sum(before * flat_hits, axis=1).reshape(slot_keys.shape)


def by_collectives(
    tokens, device_choice, local_expert, route_weight, prefill_ranks, w_gate, w_up, w_down
):
    rank_count = lax.axis_size("ep")
    own_rank = lax.axis_index("ep")
    rank_rows = tokens.shape[0]
    model_width = tokens.shape[1]
    experts_here = w_gate.shape[0]
    capacity = (DEV_TOP * rank_rows + rank_count - 1) // rank_count
    row_ids = jnp.arange(rank_rows, dtype=jnp.int32)
    is_live = (row_ids < DEC_RANK) | jnp.any(prefill_ranks == own_rank)
    pair_rank = jnp.repeat(device_choice, 2, axis=1)
    expert_keys = pair_rank * experts_here + local_expert
    positions = count_slots(device_choice, is_live, rank_count)
    send_ids = device_choice * capacity + positions
    send_count = rank_count * capacity
    pick_index = expert_keys * capacity + jnp.repeat(positions, 2, axis=1)
    block_shape = (rank_count, 1, capacity, model_width)
    slot_ids = jnp.arange(send_count, dtype=jnp.int32)
    select = jnp.any(
        (send_ids[None, :, :] == slot_ids[:, None, None]) & is_live[None, :, None], axis=2
    ).astype(jnp.bfloat16)
    outgoing = (
        jnp.dot(select, tokens, preferred_element_type=jnp.float32)
        .astype(jnp.bfloat16)
        .reshape(block_shape)
    )
    blocks = lax.all_to_all(outgoing, "ep", split_axis=0, concat_axis=0, tiled=True)
    gate_act = jnp.einsum("scd,efd->secf", blocks[:, 0], w_gate, preferred_element_type=jnp.float32)
    up_act = jnp.einsum("scd,efd->secf", blocks[:, 0], w_up, preferred_element_type=jnp.float32)
    hidden = (jax.nn.silu(gate_act) * up_act).astype(jnp.bfloat16)
    partial_value = jnp.einsum(
        "secf,efd->secd", hidden, w_down, preferred_element_type=jnp.float32
    ).astype(jnp.bfloat16)
    returned = lax.all_to_all(partial_value, "ep", split_axis=0, concat_axis=0, tiled=True)
    back_width = returned.shape[3]
    flat_back = returned.reshape(-1, back_width)
    weights = jnp.where(is_live[:, None], route_weight, jnp.zeros_like(route_weight))
    shares = jnp.zeros((rank_rows, back_width), jnp.float32)
    for pick_slot in range(TOPK):
        picked_rows = flat_back[pick_index[:, pick_slot]].astype(jnp.float32)
        shares = shares + weights[:, pick_slot : pick_slot + 1] * picked_rows
    summed = lax.psum_scatter(shares.astype(jnp.bfloat16), "tp", scatter_dimension=0, tiled=True)
    return summed


def fused_kernel(
    ranks, pairs, cuts, tokens, choice, local, route, prefill, w_gate, w_up, w_down, out,
    rows_in, mix, gate, up, down, total, half_out, half_in, side_out, side_in, far_out, far_in,
    load_sem, mix_send, mix_recv, z_send, z_recv, x_send, x_recv, c_send, c_recv,
    half_send, half_recv, side_send, side_recv, far_send, far_recv,
):
    me = lax.axis_index("ep")
    spot = lax.axis_index("tp")
    column, core = spot // CORES, spot % CORES
    partner = column * CORES + (1 - core)
    experts, hidden_here, width = w_gate.shape
    pieces, piece_rows = rows_in.shape[1], rows_in.shape[2]
    rank_rows = pieces * piece_rows

    def at_column(step):
        return ((column + step) % pairs) * CORES + core

    loads = [
        pltpu.make_async_copy(tokens, rows_in.at[me], load_sem.at[0]),
        pltpu.make_async_copy(w_gate, gate, load_sem.at[1]),
        pltpu.make_async_copy(w_up, up, load_sem.at[2]),
        pltpu.make_async_copy(w_down, down, load_sem.at[3]),
    ]
    for load in loads:
        load.start()

    barrier = pltpu.get_barrier_semaphore()
    for step in range(1, ranks):
        pl.semaphore_signal(
            barrier, inc=1, device_id={"ep": (me + step) % ranks}, device_id_type=MESH
        )
    for step in range(1, pairs):
        pl.semaphore_signal(barrier, inc=1, device_id={"tp": at_column(step)}, device_id_type=MESH)
    pl.semaphore_signal(barrier, inc=1, device_id={"tp": partner}, device_id_type=MESH)
    pl.semaphore_wait(barrier, ranks - 1 + pairs - 1 + 1)

    def remote(src, dst, send, recv, target):
        return pltpu.make_async_remote_copy(
            src_ref=src, dst_ref=dst, send_sem=send, recv_sem=recv,
            device_id=target, device_id_type=MESH,
        )

    def columns(part):
        low, size = cuts[part]
        return pl.ds(low, size)

    def mix_copy(step):
        other = (me + step) % ranks
        return remote(
            mix.at[me], mix.at[me], mix_send.at[step - 1], mix_recv.at[me], {"ep": other}
        )

    def mix_arrival(block):
        return remote(
            mix.at[block], mix.at[block], mix_send.at[0], mix_recv.at[block], {"ep": block}
        )

    def z_copy(other, part):
        piece = rows_in.at[me, spot, :, columns(part)]
        return remote(
            piece, piece, z_send.at[other, part], z_recv.at[me, part], {"ep": other}
        )

    def z_arrival(block, part):
        piece = rows_in.at[block, spot, :, columns(part)]
        return remote(
            piece, piece, z_send.at[block, part], z_recv.at[block, part], {"ep": block}
        )

    def x_copy(block, step, part):
        piece = rows_in.at[block, spot, :, columns(part)]
        return remote(
            piece, piece, x_send.at[block, step - 1, part], x_recv.at[block, step - 1, part],
            {"tp": at_column(step)},
        )

    def x_arrival(block, step, part):
        piece = rows_in.at[block, at_column(pairs - step), :, columns(part)]
        return remote(
            piece, piece, x_send.at[block, step - 1, part], x_recv.at[block, step - 1, part],
            {"tp": at_column(step)},
        )

    def c_copy(block, step, part):
        piece = rows_in.at[block, at_column(pairs - step), :, columns(part)]
        return remote(
            piece, piece, c_send.at[block, step, part], c_recv.at[block, step, part],
            {"tp": partner},
        )

    def half_copy(block, part):
        cols = columns(part)
        return remote(
            half_out.at[block, :, :, cols], half_in.at[block, :, :, cols],
            half_send.at[block, part], half_recv.at[block, part], {"tp": partner},
        )

    def side_copy(block, step, part):
        cols = columns(part)
        return remote(
            side_out.at[block, step - 1, :, cols], side_in.at[block, step - 1, :, cols],
            side_send.at[block, step - 1, part], side_recv.at[block, step - 1, part],
            {"tp": at_column(step)},
        )

    def far_copy(block, part):
        cols = columns(part)
        return remote(
            far_out.at[block, :, cols], far_in.at[me, :, cols],
            far_send.at[block, part], far_recv.at[me, part], {"ep": block},
        )

    def far_arrival(block, part):
        cols = columns(part)
        return remote(
            far_out.at[block, :, cols], far_in.at[block, :, cols],
            far_send.at[block, part], far_recv.at[block, part], {"ep": block},
        )

    parts = range(len(cuts))
    near = jnp.minimum(me, ranks - 1 - me)

    def nth(i):
        alternating = jnp.where(i % 2 == 1, me - (i + 1) // 2, me + i // 2)
        rest = jnp.where(me <= near, i, ranks - 1 - i)
        return jnp.where(i <= 2 * near, alternating, rest)

    def arrive(i):
        block = nth(i)
        for part in parts:
            z_arrival(block, part).wait_recv()
            for step in range(1, pairs):
                x_copy(block, step, part).start()
            c_copy(block, 0, part).start()

    def across(i):
        block = nth(i)
        for part in parts:
            for step in range(1, pairs):
                x_arrival(block, step, part).wait_recv()
                c_copy(block, step, part).start()

    def compute(i):
        block = nth(i)

        @pl.when(i > 0)
        def _():
            for part in parts:
                for step in range(pairs):
                    c_copy(block, step, part).wait_recv()
            mix_arrival(block).wait_recv()

        rows = rows_in[block].reshape(rank_rows, width)
        hidden = []
        for expert in range(experts):
            by_row = (((1,), (1,)), ((), ()))
            gate_act = lax.dot_general(rows, gate[expert], by_row, preferred_element_type=jnp.float32)
            up_act = lax.dot_general(rows, up[expert], by_row, preferred_element_type=jnp.float32)
            scale = jnp.broadcast_to(mix[block, pl.ds(me * experts + expert, 1), :], (LANES, rank_rows)).T
            scale = jnp.concatenate([scale] * (hidden_here // LANES), axis=1)
            act = gate_act / (1.0 + jnp.exp(-gate_act)) * up_act * scale
            hidden.append(act.astype(jnp.bfloat16))
        hidden = jnp.concatenate(hidden, axis=1)
        tile = 512 if width % 512 == 0 else LANES
        for part in parts:
            first, size = cuts[part]
            for low in range(first, first + size, min(tile, size)):
                high = min(low + tile, first + size)
                product = jnp.dot(
                    hidden,
                    down[:, :, low:high].reshape(experts * hidden_here, high - low),
                    preferred_element_type=jnp.float32,
                )
                total[block, :, :, low:high] = product.reshape(pieces, piece_rows, high - low)
            cols = columns(part)
            for col in range(pairs):
                half_out[block, col, :, cols] = total[
                    block, col * CORES + (1 - core), :, cols
                ].astype(jnp.bfloat16)
            half_copy(block, part).start()

    def merge_half(i):
        block = nth(i)
        for part in parts:
            cols = columns(part)
            half_copy(block, part).wait_recv()
            for step in range(1, pairs):
                got = half_in[block, (column + step) % pairs, :, cols].astype(jnp.float32)
                both = total[block, at_column(step), :, cols] + got
                side_out[block, step - 1, :, cols] = both.astype(jnp.bfloat16)
                side_copy(block, step, part).start()
            got = half_in[block, column, :, cols].astype(jnp.float32)
            total[block, spot, :, cols] = total[block, spot, :, cols] + got

    def merge_side(i):
        block = nth(i)
        for part in parts:
            cols = columns(part)
            acc = total[block, spot, :, cols]
            for step in range(1, pairs):
                side_copy(block, step, part).wait_recv()
                acc = acc + side_in[block, step - 1, :, cols].astype(jnp.float32)

            @pl.when(i > 0)
            def _():
                far_out[block, :, cols] = acc.astype(jnp.bfloat16)
                far_copy(block, part).start()

            @pl.when(i == 0)
            def _():
                total[block, spot, :, cols] = acc

    loads[0].wait()
    @pl.loop(1, ranks)
    def _(i):
        for part in parts:
            z_copy(nth(i), part).start()

    hit = jnp.int32(0)
    for j in range(prefill.shape[0]):
        hit = hit + jnp.where(prefill[j] == me, 1, 0)
    table = (mix.shape[1], rank_rows)
    expert_ids = lax.broadcasted_iota(jnp.int32, table, 0)
    row_ids = lax.broadcasted_iota(jnp.int32, table, 1)
    by_expert = jnp.zeros(table, jnp.float32)
    for pick in range(TOPK):
        chosen = choice[pick // 2 : pick // 2 + 1, :] * experts + local[pick : pick + 1, :]
        by_expert = by_expert + jnp.where(expert_ids == chosen, route[pick : pick + 1, :], 0.0)
    mix[me] = jnp.where(row_ids < jnp.where(hit > 0, rank_rows, DEC_RANK), by_expert, 0.0)
    for step in range(1, ranks):
        mix_copy(step).start()
    for load in loads[1:]:
        load.wait()
    arrive(1)

    @pl.loop(0, ranks)
    def _(i):
        compute(i)

        @pl.when((i == 0) & (ranks > 2))
        def _():
            arrive(2)

        @pl.when(i + 1 < ranks)
        def _():
            across(i + 1)

        @pl.when(i + 3 < ranks)
        def _():
            arrive(i + 3)

        @pl.when(i > 0)
        def _():
            merge_half(i)

        @pl.when(i > 1)
        def _():
            merge_side(i - 1)

    merge_half(0)
    merge_side(ranks - 1)
    merge_side(0)
    for part in parts:
        cols = columns(part)
        acc = total[me, spot, :, cols]
        for step in range(1, ranks):
            block = nth(step)
            far_arrival(block, part).wait_recv()
            acc = acc + far_in[block, :, cols].astype(jnp.float32)
        out[:, cols] = acc.astype(out.dtype)

    @pl.loop(0, ranks)
    def _(i):
        block = nth(i)
        for part in parts:
            half_copy(block, part).wait_send()
            for step in range(1, pairs):
                side_copy(block, step, part).wait_send()

        @pl.when(i > 0)
        def _():
            for part in parts:
                z_copy(block, part).wait_send()
                for step in range(1, pairs):
                    x_copy(block, step, part).wait_send()
                for step in range(pairs):
                    c_copy(block, step, part).wait_send()
                far_copy(block, part).wait_send()

    for step in range(1, ranks):
        mix_copy(step).wait_send()


def column_cuts(width, count):
    unit = 512 if width % 512 == 0 else LANES
    units = width // unit
    count = min(count, units)
    edges = [unit * ((units * k + count - 1) // count) for k in range(count + 1)]
    return [(low, high - low) for low, high in zip(edges, edges[1:])]


def scratch_of(ranks, pairs, cuts, experts, rank_rows, hidden_here, width):
    pieces = pairs * CORES
    piece_rows = rank_rows // pieces
    sub = (ranks * experts + 7) // 8 * 8
    parts = len(cuts)
    arrays = [
        ((ranks, pieces, piece_rows, width), jnp.bfloat16),
        ((ranks, sub, rank_rows), jnp.float32),
        ((experts, hidden_here, width), jnp.bfloat16),
        ((experts, hidden_here, width), jnp.bfloat16),
        ((experts, hidden_here, width), jnp.bfloat16),
        ((ranks, pieces, piece_rows, width), jnp.float32),
        ((ranks, pairs, piece_rows, width), jnp.bfloat16),
        ((ranks, pairs, piece_rows, width), jnp.bfloat16),
        ((ranks, pairs - 1, piece_rows, width), jnp.bfloat16),
        ((ranks, pairs - 1, piece_rows, width), jnp.bfloat16),
        ((ranks, piece_rows, width), jnp.bfloat16),
        ((ranks, piece_rows, width), jnp.bfloat16),
    ]
    sems = [
        (4,), (ranks - 1,), (ranks,), (ranks, parts), (ranks, parts),
        (ranks, pairs - 1, parts), (ranks, pairs - 1, parts),
        (ranks, pairs, parts), (ranks, pairs, parts),
        (ranks, parts), (ranks, parts),
        (ranks, pairs - 1, parts), (ranks, pairs - 1, parts), (ranks, parts), (ranks, parts),
    ]
    return arrays, sems


def byte_count(arrays):
    total = 0
    for shape, kind in arrays:
        size = jnp.dtype(kind).itemsize
        for extent in shape:
            size *= extent
        total += size
    return total


def on_device(
    tokens, device_choice, local_expert, route_weight, prefill_ranks, w_gate, w_up, w_down
):
    ranks = lax.axis_size("ep")
    spots = lax.axis_size("tp")
    rank_rows, width = tokens.shape
    experts, hidden_here, _ = w_gate.shape
    pairs = spots // CORES
    fits = False
    if (
        ranks > 1 and pairs > 1 and spots % CORES == 0 and rank_rows % (spots * 16) == 0
        and rank_rows == LANES and ranks * experts <= LANES and hidden_here % LANES == 0 and width % LANES == 0
    ):
        cuts = column_cuts(width, PARTS)
        arrays, sems = scratch_of(ranks, pairs, cuts, experts, rank_rows, hidden_here, width)
        fits = byte_count(arrays) < VMEM_BYTES * 3 // 4
    if not fits:
        return by_collectives(
            tokens, device_choice, local_expert, route_weight, prefill_ranks, w_gate, w_up, w_down
        )
    piece_rows = rank_rows // spots
    anywhere = pl.BlockSpec(memory_space=pl.ANY)
    in_smem = pl.BlockSpec(memory_space=pltpu.SMEM)
    in_vmem = pl.BlockSpec(memory_space=pltpu.VMEM)
    return pl.pallas_call(
        functools.partial(fused_kernel, ranks, pairs, cuts),
        out_shape=jax.ShapeDtypeStruct((piece_rows, width), jnp.bfloat16),
        in_specs=[anywhere, in_vmem, in_vmem, in_vmem, in_smem, anywhere, anywhere, anywhere],
        out_specs=in_vmem,
        scratch_shapes=[pltpu.VMEM(shape, kind) for shape, kind in arrays]
        + [pltpu.SemaphoreType.DMA(shape) for shape in sems],
        compiler_params=pltpu.CompilerParams(
            collective_id=0, has_side_effects=True, vmem_limit_bytes=VMEM_BYTES * 15 // 16
        ),
    )(
        tokens.reshape(spots, piece_rows, width), device_choice.T, local_expert.T,
        route_weight.T, prefill_ranks, w_gate, w_up, w_down,
    )


def solution(mesh):
    in_specs = (
        P(("groups", "ep"), None),
        P(("groups", "ep"), None),
        P(("groups", "ep"), None),
        P(("groups", "ep"), None),
        P("groups"),
        P("ep", "tp", None),
        P("ep", "tp", None),
        P("ep", "tp", None),
    )
    out_specs = P(("groups", "ep", "tp"), None)
    return jax.shard_map(
        on_device, mesh=mesh, in_specs=in_specs, out_specs=out_specs, check_vma=False
    )
```
